32 devices in a mesh: rep: 1, r: 4 (over z), s: 8 (over x, y, core).
Axes of the slice: x: 2, y: 2, z: 4, core: 2. Of those that a mesh axis runs over, the one named last changes fastest.
Arguments:
- x: bfloat16 [32, 4096, 512], P(('rep', 'r', 's'))
- dy: bfloat16 [32, 4096, 512], P(('rep', 'r', 's'))
- w_gate: bfloat16 [2, 512, 3072], P(None, 's')
- w_up: bfloat16 [2, 512, 3072], P(None, 's')
- w_down: bfloat16 [2, 3072, 512], P(None, 's')
Outputs:
- output 1: bfloat16 [32, 4096, 512], P(('rep', 'r', 's'))
- output 2: bfloat16 [2, 512, 3072], P('rep', 's')
- output 3: bfloat16 [2, 512, 3072], P('rep', 's')
- output 4: bfloat16 [2, 3072, 512], P('rep', 's')
All inputs are finite; a program needn't handle non-finite values.
Results may differ from the reference program's by a relative error of at most 0.018.
Values are sent between devices in bfloat16 or wider.
A program may use at most 2 GiB of HBM per device.

```python
import jax
import jax.numpy as jnp
from jax import lax

SEQUENCES = 32
TOKENS = 4096
D = 512
FF = 3072
LAYERS = 2
NAMES = ("w_gate", "w_up", "w_down")
SHAPES = {"w_gate": (LAYERS, D, FF), "w_up": (LAYERS, D, FF), "w_down": (LAYERS, FF, D)}


def bump(key, n, height):
    away = (jnp.arange(n, dtype=jnp.int32) - jax.random.randint(key, (), 0, n, jnp.int32)) % n
    return jnp.where(away < n // 8, height, 1.0)


def together(key, own, strength):
    shared = jax.random.normal(key, own.shape[1:], jnp.float32)
    return (own + strength * shared) * lax.rsqrt(1 + strength * strength)


def setup_inputs(seed: int = 0, part: int = 0) -> dict:
    kx, kdy, ka, kb, kz, kf, kh, kl, *kw = jax.random.split(jax.random.key(seed), 8 + len(NAMES))
    kx, kdy, ka, kb = (jax.random.fold_in(k, part) for k in (kx, kdy, ka, kb))
    shape = (SEQUENCES, TOKENS, D)
    much_x, much_dy = jax.random.uniform(kz, (2,), jnp.float32, 0.0, 1.0)
    layers = 2.0 ** jax.random.uniform(kl, (LAYERS, 1, 1), jnp.float32, -1.0, 1.0)
    x = together(ka, jax.random.normal(kx, shape, jnp.float32), much_x) * bump(kf, D, 4.0)
    dy = together(kb, jax.random.normal(kdy, shape, jnp.float32), much_dy)
    drawn = {"x": x.astype(jnp.bfloat16), "dy": (dy * (SEQUENCES * TOKENS) ** -0.5).astype(jnp.bfloat16)}
    for key, name in zip(kw, NAMES, strict=True):
        w = jax.random.normal(key, SHAPES[name], jnp.float32) * SHAPES[name][1] ** -0.5
        drawn[name] = (w * {"w_gate": 1.0, "w_up": bump(kh, FF, 4.0), "w_down": layers}[name]).astype(jnp.bfloat16)
    return drawn


def matmul(a, w):
    return jnp.dot(a, w, preferred_element_type=jnp.float32).astype(jnp.bfloat16)


def normed(h):
    wide = h.astype(jnp.float32)
    scale = lax.rsqrt(jnp.mean(wide**2, -1, keepdims=True) + 1e-6)
    return (wide * scale).astype(jnp.bfloat16)


def layer(h, w):
    a = normed(h)
    gate = jnp.dot(a, w["w_gate"], preferred_element_type=jnp.float32)
    up = jnp.dot(a, w["w_up"], preferred_element_type=jnp.float32)
    return h + matmul((jax.nn.silu(gate) * up).astype(jnp.bfloat16), w["w_down"])


def stack(weights, h):
    return lax.scan(lambda h, w: (layer(h, w), None), h, weights)[0]


def reference(x, dy, w_gate, w_up, w_down):
    weights = dict(zip(NAMES, (w_gate, w_up, w_down), strict=True))

    def take(so_far, sequence):
        h, by_y = sequence
        _, back = jax.vjp(stack, weights, h)
        by_weights, by_h = back(by_y)
        return jax.tree.map(lambda total, term: total + term.astype(jnp.float32), so_far, by_weights), by_h

    none_yet = {name: jnp.zeros(w.shape, jnp.float32) for name, w in weights.items()}
    by_weights, by_x = lax.scan(take, none_yet, (x, dy))
    return (by_x, *(by_weights[name].astype(jnp.bfloat16) for name in NAMES))
```

```python
import functools

import jax
import jax.numpy as jnp
from jax import lax
from jax.experimental import pallas as pl
from jax.experimental.pallas import tpu as pltpu
from jax.sharding import PartitionSpec as P

MESH = pl.DeviceIdType.MESH
f32, bf16 = jnp.float32, jnp.bfloat16
D, FF, F, NC, LAYERS, S, Z = 512, 3072, 512, 6, 2, 8, 4
LEAD = 3
NM = NC * LAYERS


def nn(a, b):
    return jnp.dot(a, b, preferred_element_type=f32)


def nt(a, b):
    return lax.dot_general(a, b, (((1,), (1,)), ((), ())), preferred_element_type=f32)


def normed(h):
    wide = h.astype(f32)
    return (wide * lax.rsqrt(jnp.mean(wide * wide, -1, keepdims=True) + 1e-6)).astype(bf16)


def through_norm(by_a, h):
    wide = h.astype(f32)
    scale = lax.rsqrt(jnp.mean(wide * wide, -1, keepdims=True) + 1e-6)
    along = jnp.mean(by_a * wide, -1, keepdims=True)
    return by_a * scale - wide * (scale * scale * scale * along)


def wait_for(ref, sem):
    pltpu.make_async_copy(ref, ref, sem).wait()


def kernel(T02, T1, TB, x_h, dy_h, wg_h, wu_h, wd_h,
           dx_h, ogu_h, od_h, wgu_f, wd_f, gsave, a0t_h,
           A, AT, DY, DYT, HB, ACC, WB, DW, GST, SGU,
           S1GU, S1D, R1GU, R1D, S2GU, S2D, P2GU, P2D, R2GU, R2D,
           S3GU, S3D, P3GU, P3D, R3GU, R3D, S4GU, S4D,
           st_sem, io_sem, wl_sem, g_sem, gi, di, gd, dd, ags, ads, rs):
    N = A.shape[0]
    s, z = lax.axis_index("s"), lax.axis_index("r")
    e, q = lax.rem(s, 2), lax.div(s, 2)
    qx, qy = lax.div(q, 2), lax.rem(q, 2)
    others = (2 * (1 - qx) + qy, 2 * qx + 1 - qy, 2 * (1 - qx) + 1 - qy)
    partner = {"s": 2 * q + 1 - e}

    def chip(i):
        return {"s": 2 * others[i] + e}

    def plane(i):
        return lax.rem(z + i, Z)

    def remote(src, dst, send, recv, to):
        pltpu.make_async_remote_copy(src_ref=src, dst_ref=dst, send_sem=send, recv_sem=recv, device_id=to, device_id_type=MESH).start()

    def split(kk):
        l = lax.div(kk, NC)
        c = lax.rem(kk, NC)
        return l, c, lax.rem(c, 2), lax.div(c, 2)

    def send_own(kk):
        l, c, h, j = split(kk)
        rows = pl.ds(pl.multiple_of(64 * s, 64), 64)
        src, dst = SGU.at[l, c], wgu_f.at[l, c, :, rows, :]
        for i in range(3):
            remote(src, dst, ags.at[kk], gi.at[kk], chip(i))
        remote(src, dst, ags.at[kk], gd.at[kk], partner)
        pltpu.make_async_copy(src, dst, gi.at[kk]).start()

        @pl.when(h == e)
        def _():
            src = wd_h.at[l, pl.ds(pl.multiple_of(128 * j, 128), 128), :]
            dst = wd_f.at[l, c, pl.ds(pl.multiple_of(128 * q, 128), 128), :]
            for i in range(3):
                remote(src, dst, ads.at[kk], di.at[kk], chip(i))
            remote(src, dst, ads.at[kk], dd.at[kk], partner)
            pltpu.make_async_copy(src, dst, di.at[kk]).start()

    def forward(kk):
        l, c, h, j = split(kk)
        wait_for(wgu_f.at[l, c, :, pl.ds(0, 256), :], gi.at[kk])
        for i in range(3):
            block = wgu_f.at[l, c, :, pl.ds(pl.multiple_of(64 * (2 * others[i] + e), 64), 64), :]
            remote(block, block, ags.at[kk], gd.at[kk], partner)

        @pl.when(h == e)
        def _():
            wait_for(wd_f.at[l, c], di.at[kk])
            for i in range(3):
                block = wd_f.at[l, c, pl.ds(pl.multiple_of(128 * others[i], 128), 128), :]
                remote(block, block, ads.at[kk], dd.at[kk], partner)

    def arrive(kk):
        l, c, h, j = split(kk)
        wait_for(wgu_f.at[l, c, :, pl.ds(0, 256), :], gd.at[kk])

        @pl.when(h != e)
        def _():
            wait_for(wd_f.at[l, c], dd.at[kk])

    def load(kk):
        l = lax.rem(lax.div(kk, NC), LAYERS)
        c, slot = lax.rem(kk, NC), lax.rem(kk, 2)
        pltpu.make_async_copy(wgu_f.at[l, c], WB.at[slot, pl.ds(0, 2)], wl_sem.at[slot]).start()
        pltpu.make_async_copy(wd_f.at[l, c], WB.at[slot, 2], wl_sem.at[slot]).start()

    def loaded(kk):
        slot = lax.rem(kk, 2)
        wait_for(WB.at[slot], wl_sem.at[slot])

    def sent_all(kk):
        l, c, h, j = split(kk)
        wait_for(wgu_f.at[l, c, :, pl.ds(0, 448), :], ags.at[kk])

        @pl.when(h == e)
        def _():
            wait_for(wgu_f.at[l, c, :, pl.ds(0, 448), :], ads.at[kk])

    def place(m):
        l = 1 - lax.div(m, NC)
        c = lax.rem(m, NC)
        return l, c, lax.rem(c, 2), lax.div(c, 2), lax.rem(m, 2)

    def rows64(block):
        return pl.ds(pl.multiple_of(64 * block, 64), 64)

    def pair_send(m):
        l, c, h, j, sl = place(m)

        @pl.when(m >= 1)
        def _():
            wait_for(S1GU, rs.at[0, m - 1])
        for p in range(4):
            for n in range(2):
                S1GU[p, n] = DW[sl, n, rows64(2 * p + 1 - e), :].astype(bf16)
        remote(S1GU, R1GU.at[sl], rs.at[0, m], rs.at[1, m], partner)

        @pl.when(h != e)
        def _():
            @pl.when(m >= 2)
            def _():
                wait_for(S1D, rs.at[2, m - 2])
            for p in range(4):
                S1D[p] = DW[sl, 2, :, 128 * p:128 * p + 128].astype(bf16)
            remote(S1D, R1D, rs.at[2, m], rs.at[3, m], partner)

    def pair_sum(m):
        l, c, h, j, sl = place(m)
        wait_for(R1GU.at[sl], rs.at[1, m])

        @pl.when(m >= 1)
        def _():
            wait_for(R2GU.at[0], rs.at[4, m - 1])
        for p in range(4):
            for n in range(2):
                S2GU[p, n] = (DW[sl, n, rows64(2 * p + e), :] + R1GU[sl, p, n].astype(f32)).astype(bf16)
        for n in range(2):
            P2GU[n] = DW[sl, n, rows64(2 * q + e), :] + R1GU[sl, q, n].astype(f32)
        for i in range(3):
            remote(S2GU.at[others[i]], R2GU.at[sl, i], rs.at[4, m], rs.at[5, m], chip(i))

        @pl.when(h == e)
        def _():
            wait_for(R1D, rs.at[3, m])

            @pl.when(m >= 2)
            def _():
                wait_for(R2D, rs.at[6, m - 2])
            for p in range(4):
                total = DW[sl, 2, :, 128 * p:128 * p + 128] + R1D[p].astype(f32)
                S2D[p] = total.astype(bf16)

                @pl.when(q == p)
                def _():
                    P2D[...] = total
            for i in range(3):
                remote(S2D.at[others[i]], R2D.at[i], rs.at[6, m], rs.at[7, m], chip(i))

    def plane_sum(m):
        l, c, h, j, sl = place(m)
        wait_for(R2GU.at[sl], rs.at[5, m])

        @pl.when(m >= 1)
        def _():
            wait_for(R3GU.at[0], rs.at[8, m - 1])
        for p in range(4):
            k = slice(16 * p, 16 * p + 16)
            total = P2GU[:, k, :]
            for i in range(3):
                total += R2GU[sl, i, :, k, :].astype(f32)
            S3GU[p] = total.astype(bf16)

            @pl.when(z == p)
            def _():
                P3GU[...] = total
        for i in range(1, 4):
            remote(S3GU.at[plane(i)], R3GU.at[sl, i - 1], rs.at[8, m], rs.at[9, m], {"r": plane(i)})

        @pl.when(h == e)
        def _():
            wait_for(R2D, rs.at[7, m])

            @pl.when(m >= 2)
            def _():
                wait_for(R3D, rs.at[10, m - 2])
            for p in range(4):
                k = slice(128 * p, 128 * p + 128)
                total = P2D[k, :]
                for i in range(3):
                    total += R2D[i, k, :].astype(f32)
                S3D[p] = total.astype(bf16)

                @pl.when(z == p)
                def _():
                    P3D[...] = total
            for i in range(1, 4):
                remote(S3D.at[plane(i)], R3D.at[i - 1], rs.at[10, m], rs.at[11, m], {"r": plane(i)})

    def last_sum(m):
        l, c, h, j, sl = place(m)
        wait_for(R3GU.at[sl], rs.at[9, m])

        @pl.when(m >= 1)
        def _():
            wait_for(S3GU, rs.at[12, m - 1])
        S4GU[...] = (P3GU[...] + R3GU[sl, 0].astype(f32) + R3GU[sl, 1].astype(f32) + R3GU[sl, 2].astype(f32)).astype(bf16)
        dst = ogu_h.at[l, c, z]
        for i in range(1, 4):
            remote(S4GU, dst, rs.at[12, m], rs.at[13, m], {"r": plane(i)})
        pltpu.make_async_copy(S4GU, dst, rs.at[12, m]).start()

        @pl.when(h == e)
        def _():
            wait_for(R3D, rs.at[11, m])

            @pl.when(m >= 2)
            def _():
                wait_for(S3D, rs.at[14, m - 2])
            S4D[...] = (P3D[...] + R3D[0].astype(f32) + R3D[1].astype(f32) + R3D[2].astype(f32)).astype(bf16)
            dst = od_h.at[l, j, z]
            for i in range(1, 4):
                remote(S4D, dst, rs.at[14, m], rs.at[15, m], {"r": plane(i)})
            pltpu.make_async_copy(S4D, dst, rs.at[14, m]).start()

    def ended(m):
        l, c, h, j, sl = place(m)
        wait_for(R3GU.at[0], rs.at[13, m])

        @pl.when(h == e)
        def _():
            wait_for(R3D, rs.at[15, m])

    def hooks(kk, t, NT, gathers, reduces):
        at = [NT * i // 4 for i in range(4)]

        @pl.when(t == at[0])
        def _():
            loaded(kk)
            if reduces:
                @pl.when(kk >= NC + 2)
                def _():
                    plane_sum(kk - NC - 2)

                @pl.when(kk >= NC + 1)
                def _():
                    pair_send(kk - NC - 1)

        @pl.when(t == at[1])
        def _():
            if gathers:
                @pl.when(kk + 1 < NM)
                def _():
                    forward(kk + 1)

                @pl.when(kk + LEAD < NM)
                def _():
                    send_own(kk + LEAD)
            if reduces:
                @pl.when(kk >= NC + 1)
                def _():
                    pair_sum(kk - NC - 1)

        if reduces:
            @pl.when(t == at[2])
            def _():
                @pl.when(kk >= NC + 2)
                def _():
                    last_sum(kk - NC - 2)

        @pl.when(t == at[3])
        def _():
            if gathers:
                @pl.when(kk + 1 < NM)
                def _():
                    arrive(kk + 1)

            @pl.when(kk + 1 < 3 * NC)
            def _():
                load(kk + 1)

    def tile(t, T):
        return pl.ds(pl.multiple_of(t * T, T), T)

    xin = pltpu.make_async_copy(x_h, HB, io_sem.at[0])
    dyin = pltpu.make_async_copy(dy_h, DY, io_sem.at[1])
    for l in range(LAYERS):
        def stage(c, _):
            h, j = lax.rem(c, 2), lax.div(c, 2)
            for p in range(4):
                cols = pl.ds(pl.multiple_of(384 * (2 * p + h) + 128 * j, 128), 128)
                for n, w in enumerate((wg_h, wu_h)):
                    pltpu.make_async_copy(w.at[l, :, cols], SGU.at[l, c, n, :, pl.ds(128 * p, 128)], st_sem.at[l]).start()
            return 0
        lax.fori_loop(0, NC, stage, 0)
    xin.start()
    dyin.start()
    barrier = pltpu.get_barrier_semaphore()
    peers = [partner] + [chip(i) for i in range(3)] + [{"r": plane(i)} for i in range(1, 4)]
    for to in peers:
        pl.semaphore_signal(barrier, 1, device_id=to, device_id_type=MESH)
    wait_for(SGU.at[0], st_sem.at[0])
    wait_for(SGU.at[1], st_sem.at[1])
    pl.semaphore_wait(barrier, len(peers))
    for kk in range(LEAD):
        send_own(jnp.int32(kk))
    xin.wait()
    dyin.wait()

    def prepare(t, _):
        r = tile(t, TB)
        a = normed(HB[r, :])
        A[r, :] = a
        AT[:, r] = a.T
        DYT[:, r] = DY[r, :].T
        ACC[r, :] = jnp.zeros((TB, D), f32)
        return 0

    lax.fori_loop(0, N // TB, prepare, 0)
    keep = pltpu.make_async_copy(AT, a0t_h, io_sem.at[2])
    keep.start()
    forward(jnp.int32(0))
    arrive(jnp.int32(0))
    load(jnp.int32(0))

    NT = N // T02

    def save(i, go):
        sl = lax.rem(i, 2)
        c, t = lax.div(i, NT), lax.rem(i, NT)
        cp = pltpu.make_async_copy(GST.at[sl], gsave.at[c, :, tile(t, T02), :], g_sem.at[sl])
        cp.start() if go else cp.wait()

    def phase0(i, _):
        kk, t, sl = lax.div(i, NT), lax.rem(i, NT), lax.rem(i, 2)
        hooks(kk, t, NT, True, False)

        @pl.when(i >= 2)
        def _():
            save(i - 2, False)
        w, r = lax.rem(kk, 2), tile(t, T02)
        a = A[r, :]
        g, u = nn(a, WB[w, 0]), nn(a, WB[w, 1])
        GST[sl, 0] = g
        GST[sl, 1] = u
        p = (g / (1.0 + jnp.exp(-g)) * u).astype(bf16)
        ACC[r, :] += nn(p, WB[w, 2])
        save(i, True)
        return 0

    lax.fori_loop(0, NC * NT, phase0, 0)
    save(jnp.int32(NC * NT - 2), False)
    save(jnp.int32(NC * NT - 1), False)
    keep.wait()

    def between(t, _):
        r = tile(t, TB)
        h = (HB[r, :].astype(f32) + ACC[r, :].astype(bf16).astype(f32)).astype(bf16)
        HB[r, :] = h
        a = normed(h)
        A[r, :] = a
        AT[:, r] = a.T
        ACC[r, :] = jnp.zeros((TB, D), f32)
        return 0

    lax.fori_loop(0, N // TB, between, 0)

    def backward(kk, t, T, g, u):
        w, r, sl = lax.rem(kk, 2), tile(t, T), lax.rem(kk + 1, 2)
        sl = lax.rem(kk, 2)
        by_p = nt(DY[r, :], WB[w, 2]).astype(bf16).astype(f32)
        sig = 1.0 / (1.0 + jnp.exp(-g))
        act = g * sig
        p = (act * u).astype(bf16)
        by_u = (by_p * act).astype(bf16)
        by_g = (by_p * u * (sig + act * (1.0 - sig))).astype(bf16)
        ACC[r, :] += nt(by_g, WB[w, 0]) + nt(by_u, WB[w, 1])
        first = t == 0
        DW[sl, 0] = jnp.where(first, 0.0, DW[sl, 0]) + nn(AT[:, r], by_g)
        DW[sl, 1] = jnp.where(first, 0.0, DW[sl, 1]) + nn(AT[:, r], by_u)
        DW[sl, 2] = jnp.where(first, 0.0, DW[sl, 2]) + nn(DYT[:, r], p)

    NT1 = N // T1

    def phase1(i, _):
        kk, t = NC + lax.div(i, NT1), lax.rem(i, NT1)
        hooks(kk, t, NT1, True, True)
        w, a = lax.rem(kk, 2), A[tile(t, T1), :]
        backward(kk, t, T1, nn(a, WB[w, 0]), nn(a, WB[w, 1]))
        return 0

    lax.fori_loop(0, NC * NT1, phase1, 0)
    again = pltpu.make_async_copy(a0t_h, AT, io_sem.at[2])
    again.start()

    def fetch(i, go):
        sl = lax.rem(i, 2)
        c, t = lax.div(i, NT), lax.rem(i, NT)
        cp = pltpu.make_async_copy(gsave.at[c, :, tile(t, T02), :], GST.at[sl], g_sem.at[sl])
        cp.start() if go else cp.wait()

    fetch(jnp.int32(0), True)

    def turn(t, _):
        r = tile(t, TB)
        by_a = ACC[r, :].astype(bf16).astype(f32)
        by_h = (DY[r, :].astype(f32) + through_norm(by_a, HB[r, :]).astype(bf16).astype(f32)).astype(bf16)
        DY[r, :] = by_h
        DYT[:, r] = by_h.T
        ACC[r, :] = jnp.zeros((TB, D), f32)
        return 0

    lax.fori_loop(0, N // TB, turn, 0)
    xin.start()
    again.wait()

    def phase2(i, _):
        kk, t, sl = 2 * NC + lax.div(i, NT), lax.rem(i, NT), lax.rem(i, 2)
        hooks(kk, t, NT, False, True)

        @pl.when(i + 1 < NC * NT)
        def _():
            fetch(i + 1, True)
        fetch(i, False)
        backward(kk, t, T02, GST[sl, 0], GST[sl, 1])
        return 0

    lax.fori_loop(0, NC * NT, phase2, 0)
    plane_sum(jnp.int32(NM - 2))
    pair_send(jnp.int32(NM - 1))
    xin.wait()

    def out(t):
        return pltpu.make_async_copy(DY.at[tile(t, TB)], dx_h.at[tile(t, TB)], io_sem.at[1])

    def finish(t, _):
        r = tile(t, TB)
        by_a = ACC[r, :].astype(bf16).astype(f32)
        DY[r, :] = (DY[r, :].astype(f32) + through_norm(by_a, HB[r, :]).astype(bf16).astype(f32)).astype(bf16)
        return 0

    half = N // TB // 2
    lax.fori_loop(0, half, finish, 0)
    pair_sum(jnp.int32(NM - 1))
    last_sum(jnp.int32(NM - 2))
    lax.fori_loop(half, N // TB, finish, 0)
    dxout = pltpu.make_async_copy(DY, dx_h, io_sem.at[1])
    dxout.start()
    plane_sum(jnp.int32(NM - 1))
    last_sum(jnp.int32(NM - 1))

    def settle(kk, _):
        sent_all(kk)
        ended(kk)
        return 0

    lax.fori_loop(0, NM, settle, 0)
    wait_for(S1GU, rs.at[0, NM - 1])
    wait_for(R2GU.at[0], rs.at[4, NM - 1])
    wait_for(R3GU.at[0], rs.at[8, NM - 1])
    wait_for(S3GU, rs.at[12, NM - 1])

    def last_d(m):
        wait_for(R2D, rs.at[6, m])
        wait_for(R3D, rs.at[10, m])
        wait_for(S3D, rs.at[14, m])

    @pl.when(e == 0)
    def _():
        wait_for(S1D, rs.at[2, NM - 1])
        last_d(NM - 2)

    @pl.when(e == 1)
    def _():
        wait_for(S1D, rs.at[2, NM - 2])
        last_d(NM - 1)
    dxout.wait()


def solution(mesh, T02=512, T1=1024, TB=512):
    def step(x, dy, w_gate, w_up, w_down):
        N = x.shape[1]
        hbm = pl.BlockSpec(memory_space=pl.ANY)
        sds = jax.ShapeDtypeStruct
        v, dma = pltpu.VMEM, pltpu.SemaphoreType.DMA
        dx, ogu, od, *_ = pl.pallas_call(
            functools.partial(kernel, min(T02, N), min(T1, N), min(TB, N)),
            name="step",
            out_shape=[
                sds((N, D), bf16), sds((LAYERS, NC, Z, 2, 16, F), bf16), sds((LAYERS, 3, Z, 128, 128), bf16),
                sds((LAYERS, NC, 2, D, F), bf16), sds((LAYERS, NC, F, D), bf16), sds((NC, 2, N, F), f32), sds((D, N), bf16),
            ],
            in_specs=[hbm] * 5,
            out_specs=[hbm] * 7,
            scratch_shapes=[
                v((N, D), bf16), v((D, N), bf16), v((N, D), bf16), v((D, N), bf16), v((N, D), bf16), v((N, D), f32),
                v((2, 3, 512, 512), bf16), v((2, 3, 512, 512), f32), v((2, 2, min(T02, N), F), f32), v((LAYERS, NC, 2, 64, F), bf16),
                v((4, 2, 64, F), bf16), v((4, D, 128), bf16), v((2, 4, 2, 64, F), bf16), v((4, D, 128), bf16),
                v((4, 2, 64, F), bf16), v((4, D, 128), bf16), v((2, 64, F), f32), v((D, 128), f32), v((2, 3, 2, 64, F), bf16), v((3, D, 128), bf16),
                v((4, 2, 16, F), bf16), v((4, 128, 128), bf16), v((2, 16, F), f32), v((128, 128), f32), v((2, 3, 2, 16, F), bf16), v((3, 128, 128), bf16),
                v((2, 16, F), bf16), v((128, 128), bf16),
                dma((2,)), dma((3,)), dma((2,)), dma((2,)), dma((NM,)), dma((NM,)), dma((NM,)), dma((NM,)), dma((NM,)), dma((NM,)), dma((16, NM)),
            ],
            compiler_params=pltpu.CompilerParams(collective_id=0, has_side_effects=True, vmem_limit_bytes=67043328),
        )(x[0], dy[0], w_gate, w_up, w_down)
        gu = ogu.reshape(LAYERS, 3, 2, Z, 2, 16, 4, 128).transpose(4, 0, 3, 5, 6, 2, 1, 7).reshape(2, LAYERS, 64, FF)
        down = od.transpose(0, 1, 4, 2, 3).reshape(LAYERS, 384, D)
        return dx[None], gu[0], gu[1], down

    states, cut = P(("rep", "r", "s"), None, None), P(None, "s", None)
    return jax.shard_map(
        step,
        mesh=mesh,
        in_specs=(states, states) + (cut,) * 3,
        out_specs=(states,) + (P("rep", "s", None),) * 3,
        check_vma=False,
    )
```

```python
import functools

import jax
import jax.numpy as jnp
from jax import lax
from jax.experimental import pallas as pl
from jax.experimental.pallas import tpu as pltpu
from jax.sharding import PartitionSpec as P

MESH = pl.DeviceIdType.MESH
DOWN = 2
LANES, ROWS, QUARTER = 128, 64, 16
PAIR_OUT, PAIR_IN, PLANE_OUT, PLANE_IN, ACROSS_OUT, ACROSS_IN, ROUND_OUT, ROUND_IN = range(8)
f32, bf16 = jnp.float32, jnp.bfloat16
D, FF, F, NC, LAYERS, S, Z = 512, 3072, 512, 6, 2, 8, 4
SUB = 512
NM = NC * LAYERS


def odd(n):
    return lax.rem(n, 2)


def nn(a, b):
    return jnp.dot(a, b, preferred_element_type=f32)


def nt(a, b):
    return lax.dot_general(a, b, (((1,), (1,)), ((), ())), preferred_element_type=f32)


def normed(h):
    wide = h.astype(f32)
    return (wide * lax.rsqrt(jnp.mean(wide * wide, -1, keepdims=True) + 1e-6)).astype(bf16)


def through_norm(by_a, h):
    wide = h.astype(f32)
    scale = lax.rsqrt(jnp.mean(wide * wide, -1, keepdims=True) + 1e-6)
    along = jnp.mean(by_a * wide, -1, keepdims=True)
    return by_a * scale - wide * (scale * scale * scale * along)


def wait_for(ref, sem):
    pltpu.make_async_copy(ref, ref, sem).wait()


def kernel(T, TB, x_h, dy_h, wg_h, wu_h, wd_h,
           dx_h, ogu_h, od_h, wgu_f, wd_f, gsave_h, a0t_h,
           A, AT, DY, DYT, HB, ACC, WB, DW, GST, SGU,
           S1GU, S1D, R1GU, R1D, S2GU, S2D, P2GU, P2D, R2GU, R2D,
           S3GU, S3D, P3GU, P3D, R3GU, R3D, S4GU, S4D,
           st_sem, io_sem, wl_sem, g_sem, gi, di, dz, gd, dd, ags, ads, x_sem, rs):
    N = A.shape[0]
    s, z = lax.axis_index("s"), lax.axis_index("r")
    e, q = odd(s), lax.div(s, 2)
    qx, qy = lax.div(q, 2), odd(q)
    others = (2 * (1 - qx) + qy, 2 * qx + 1 - qy, 2 * (1 - qx) + 1 - qy)
    partner = {"s": 2 * q + 1 - e}

    def chip(i):
        return {"s": 2 * others[i] + e}

    def plane(i):
        return lax.rem(z + i, Z)

    def remote(src, dst, send, recv, to):
        pltpu.make_async_remote_copy(src_ref=src, dst_ref=dst, send_sem=send, recv_sem=recv, device_id=to, device_id_type=MESH).start()

    def split(kk):
        l = lax.div(kk, NC)
        c = lax.rem(kk, NC)
        return l, c, odd(c), lax.div(c, 2)

    def own_gu(kk):
        l, c, h, j = split(kk)
        wait_for(SGU.at[c], st_sem.at[kk])
        src, dst = SGU.at[c], wgu_f.at[l, c, :, pl.ds(pl.multiple_of(ROWS * s, ROWS), ROWS), :]
        for i in range(3):
            remote(src, dst, ags.at[kk], gi.at[kk], chip(i))
        remote(src, dst, ags.at[kk], gd.at[kk], partner)
        pltpu.make_async_copy(src, dst, gi.at[kk]).start()

    def forward_gu(kk):
        l, c, h, j = split(kk)
        wait_for(wgu_f.at[l, c, :, pl.ds(0, 256), :], gi.at[kk])
        for i in range(3):
            block = wgu_f.at[l, c, :, pl.ds(pl.multiple_of(ROWS * (2 * others[i] + e), ROWS), ROWS), :]
            remote(block, block, ags.at[kk], gd.at[kk], partner)

    def when_mine(kk, do):
        l, c, h, j = split(kk)

        @pl.when(h == e)
        def _():
            do(l, c, j)

    def own_d(kk):
        def do(l, c, j):
            src, dst = wd_h.at[l, pl.ds(pl.multiple_of(LANES * j + 32 * z, 32), 32), :], wd_f.at[l, c, q, z]
            for i in range(3):
                remote(src, dst, ads.at[kk], di.at[kk], chip(i))
            pltpu.make_async_copy(src, dst, di.at[kk]).start()
        when_mine(kk, do)

    def across_d(kk):
        def do(l, c, j):
            block = wd_f.at[l, c, :, z]
            wait_for(block, di.at[kk])
            for i in range(1, 4):
                remote(block, block, ads.at[kk], dz.at[kk], {"r": plane(i)})
        when_mine(kk, do)

    def forward_d(kk):
        def do(l, c, j):
            wait_for(wd_f.at[l, c, pl.ds(0, 3)], dz.at[kk])
            remote(wd_f.at[l, c], wd_f.at[l, c], ads.at[kk], dd.at[kk], partner)
        when_mine(kk, do)

    def arrive(kk):
        l, c, h, j = split(kk)
        wait_for(wgu_f.at[l, c, :, pl.ds(0, 256), :], gd.at[kk])

        @pl.when(h != e)
        def _():
            wait_for(wd_f.at[l, c], dd.at[kk])

    def stage(kk, _):
        l, c, h, j = split(kk)
        for p in range(4):
            cols = pl.ds(pl.multiple_of(384 * (2 * p + h) + LANES * j, LANES), LANES)
            for n, w in enumerate((wg_h, wu_h)):
                pltpu.make_async_copy(w.at[l, :, cols], SGU.at[c, n, :, pl.ds(LANES * p, LANES)], st_sem.at[kk]).start()
        return 0

    def gather_step(k):
        def go(do, kk):
            @pl.when(kk < NM)
            def _():
                do(kk)
        go(forward_gu, k)

        @pl.when(jnp.logical_and(k >= NC - 3, k + 3 < NM))
        def _():
            wait_for(wgu_f.at[0, 0, :, pl.ds(0, 448), :], ags.at[k + 3 - NC])
            stage(k + 3, 0)
        go(own_d, k + 3)
        go(own_gu, k + 2)
        go(across_d, k + 1)
        go(forward_d, k)

    def load(kk):
        l = lax.rem(lax.div(kk, NC), LAYERS)
        c, slot = lax.rem(kk, NC), odd(kk)
        pltpu.make_async_copy(wgu_f.at[l, c], WB.at[slot, pl.ds(0, 2)], wl_sem.at[slot]).start()
        for p in range(4):
            for y in range(Z):
                pltpu.make_async_copy(wd_f.at[l, c, p, y], WB.at[slot, 2, pl.ds(LANES * p + 32 * y, 32)], wl_sem.at[slot]).start()

    def loaded(kk):
        slot = odd(kk)
        wait_for(WB.at[slot], wl_sem.at[slot])

    def sent_all(kk):
        l, c, h, j = split(kk)
        @pl.when(kk >= NC)
        def _():
            wait_for(wgu_f.at[l, c, :, pl.ds(0, 448), :], ags.at[kk])

        @pl.when(h == e)
        def _():
            wait_for(wgu_f.at[l, c, :, pl.ds(0, 496), :], ads.at[kk])

    def place(m):
        l = 1 - lax.div(m, NC)
        c = lax.rem(m, NC)
        return l, c, odd(c), lax.div(c, 2), odd(m)

    def rows64(block):
        return pl.ds(pl.multiple_of(ROWS * block, ROWS), ROWS)

    def pair_send_gu(m, n):
        sl = odd(m)

        @pl.when(m >= 1)
        def _():
            wait_for(S1GU.at[n], rs.at[PAIR_OUT, n, 1 - sl])
        for p in range(4):
            S1GU[n, p] = DW[sl, n, rows64(2 * p + 1 - e), :].astype(bf16)
        remote(S1GU.at[n], R1GU.at[sl, n], rs.at[PAIR_OUT, n, sl], rs.at[PAIR_IN, n, sl], partner)

    def pair_send_d(m):
        l, c, h, j, sl = place(m)

        @pl.when(h != e)
        def _():
            @pl.when(m >= 2)
            def _():
                wait_for(S1D, rs.at[PAIR_OUT, DOWN, sl])
            for p in range(4):
                S1D[p] = DW[sl, 2, :, LANES * p:LANES * p + LANES].astype(bf16)
            remote(S1D, R1D, rs.at[PAIR_OUT, DOWN, sl], rs.at[PAIR_IN, DOWN, sl], partner)

    def pair_sum_gu(m, n):
        sl = odd(m)
        wait_for(R1GU.at[sl, n], rs.at[PAIR_IN, n, sl])

        @pl.when(m >= 1)
        def _():
            wait_for(R2GU.at[0, n], rs.at[PLANE_OUT, n, 1 - sl])
        for p in range(4):
            S2GU[n, p] = (DW[sl, n, rows64(2 * p + e), :] + R1GU[sl, n, p].astype(f32)).astype(bf16)
        P2GU[n] = DW[sl, n, rows64(2 * q + e), :] + R1GU[sl, n, q].astype(f32)
        for i in range(3):
            remote(S2GU.at[n, others[i]], R2GU.at[sl, n, i], rs.at[PLANE_OUT, n, sl], rs.at[PLANE_IN, n, sl], chip(i))

    def pair_sum_d(m):
        l, c, h, j, sl = place(m)

        @pl.when(h == e)
        def _():
            wait_for(R1D, rs.at[PAIR_IN, DOWN, sl])

            @pl.when(m >= 2)
            def _():
                wait_for(R2D, rs.at[PLANE_OUT, DOWN, sl])
            for p in range(4):
                total = DW[sl, 2, :, LANES * p:LANES * p + LANES] + R1D[p].astype(f32)
                S2D[p] = total.astype(bf16)

                @pl.when(q == p)
                def _():
                    P2D[...] = total
            for i in range(3):
                remote(S2D.at[others[i]], R2D.at[i], rs.at[PLANE_OUT, DOWN, sl], rs.at[PLANE_IN, DOWN, sl], chip(i))

    def ended_gu(m, n):
        wait_for(R3GU.at[0, n], rs.at[ROUND_IN, n, odd(m)])

    def ended_d(m):
        l, c, h, j, sl = place(m)

        @pl.when(h == e)
        def _():
            wait_for(R3D, rs.at[ROUND_IN, DOWN, sl])

    def plane_gu(m, n):
        sl = odd(m)
        wait_for(R2GU.at[sl, n], rs.at[PLANE_IN, n, sl])

        @pl.when(m >= 1)
        def _():
            wait_for(R3GU.at[0, n], rs.at[ACROSS_OUT, n, 1 - sl])

        @pl.when(m >= 2)
        def _():
            ended_gu(m - 2, n)
        for p in range(4):
            k = slice(QUARTER * p, QUARTER * p + QUARTER)
            total = P2GU[n, k, :]
            for i in range(3):
                total += R2GU[sl, n, i, k, :].astype(f32)
            S3GU[n, p] = total.astype(bf16)

            @pl.when(z == p)
            def _():
                P3GU[n] = total
        for i in range(1, 4):
            remote(S3GU.at[n, plane(i)], R3GU.at[sl, n, i - 1], rs.at[ACROSS_OUT, n, sl], rs.at[ACROSS_IN, n, sl], {"r": plane(i)})

    def plane_d(m):
        l, c, h, j, sl = place(m)

        @pl.when(h == e)
        def _():
            wait_for(R2D, rs.at[PLANE_IN, DOWN, sl])

            @pl.when(m >= 2)
            def _():
                wait_for(R3D, rs.at[ACROSS_OUT, DOWN, sl])
                ended_d(m - 2)
            for p in range(4):
                k = slice(LANES * p, LANES * p + LANES)
                total = P2D[k, :]
                for i in range(3):
                    total += R2D[i, k, :].astype(f32)
                S3D[p] = total.astype(bf16)

                @pl.when(z == p)
                def _():
                    P3D[...] = total
            for i in range(1, 4):
                remote(S3D.at[plane(i)], R3D.at[i - 1], rs.at[ACROSS_OUT, DOWN, sl], rs.at[ACROSS_IN, DOWN, sl], {"r": plane(i)})

    def last_gu(m, n):
        l, c, h, j, sl = place(m)
        wait_for(R3GU.at[sl, n], rs.at[ACROSS_IN, n, sl])

        @pl.when(m >= 1)
        def _():
            wait_for(S3GU.at[n], rs.at[ROUND_OUT, n, 1 - sl])
        S4GU[n] = (P3GU[n] + R3GU[sl, n, 0].astype(f32) + R3GU[sl, n, 1].astype(f32) + R3GU[sl, n, 2].astype(f32)).astype(bf16)
        dst = ogu_h.at[l, c, z, n]
        for i in range(1, 4):
            remote(S4GU.at[n], dst, rs.at[ROUND_OUT, n, sl], rs.at[ROUND_IN, n, sl], {"r": plane(i)})
        pltpu.make_async_copy(S4GU.at[n], dst, rs.at[ROUND_OUT, n, sl]).start()

    def last_d(m):
        l, c, h, j, sl = place(m)

        @pl.when(h == e)
        def _():
            wait_for(R3D, rs.at[ACROSS_IN, DOWN, sl])

            @pl.when(m >= 2)
            def _():
                wait_for(S3D, rs.at[ROUND_OUT, DOWN, sl])
            S4D[...] = (P3D[...] + R3D[0].astype(f32) + R3D[1].astype(f32) + R3D[2].astype(f32)).astype(bf16)
            dst = od_h.at[l, j, z]
            for i in range(1, 4):
                remote(S4D, dst, rs.at[ROUND_OUT, DOWN, sl], rs.at[ROUND_IN, DOWN, sl], {"r": plane(i)})
            pltpu.make_async_copy(S4D, dst, rs.at[ROUND_OUT, DOWN, sl]).start()

    def whole(gu, d, m):
        gu(m, 0)
        gu(m, 1)
        d(m)

    def pair_send(m):
        whole(pair_send_gu, pair_send_d, m)

    def pair_sum(m):
        whole(pair_sum_gu, pair_sum_d, m)

    def plane_sum(m):
        whole(plane_gu, plane_d, m)

    def last_sum(m):
        whole(last_gu, last_d, m)

    def first_half(kk):
        @pl.when(kk >= NC + 3)
        def _():
            last_sum(kk - NC - 3)

        @pl.when(kk >= NC + 1)
        def _():
            pair_send(kk - NC - 1)

    def second_half(kk):
        @pl.when(kk >= NC + 2)
        def _():
            plane_sum(kk - NC - 2)

        @pl.when(kk >= NC + 1)
        def _():
            pair_sum(kk - NC - 1)

    def tile(t, T):
        return pl.ds(pl.multiple_of(t * T, T), T)

    xin = pltpu.make_async_copy(x_h, HB, io_sem.at[0])
    dyin = pltpu.make_async_copy(dy_h, DY, io_sem.at[1])
    barrier = pltpu.get_barrier_semaphore()
    peers = [partner] + [chip(i) for i in range(3)] + [{"r": plane(i)} for i in range(1, 4)]
    for to in peers:
        pl.semaphore_signal(barrier, 1, device_id=to, device_id_type=MESH)
    stage(jnp.int32(0), 0)
    xin.start()
    dyin.start()
    lax.fori_loop(1, NC, stage, 0)
    pl.semaphore_wait(barrier, len(peers))
    own_d(jnp.int32(0))
    own_gu(jnp.int32(0))
    own_d(jnp.int32(1))
    own_d(jnp.int32(2))
    xin.wait()
    dyin.wait()

    def prepare(t, _):
        r = tile(t, TB)
        a = normed(HB[r, :])
        A[r, :] = a
        AT[:, r] = a.T
        DYT[:, r] = DY[r, :].T
        ACC[r, :] = jnp.zeros((TB, D), f32)
        return 0

    across_d(jnp.int32(0))
    lax.fori_loop(0, N // TB, prepare, 0)
    keep = pltpu.make_async_copy(AT, a0t_h, io_sem.at[2])
    keep.start()
    forward_gu(jnp.int32(0))
    own_gu(jnp.int32(1))
    own_d(jnp.int32(3))
    own_gu(jnp.int32(2))
    across_d(jnp.int32(1))
    forward_d(jnp.int32(0))
    arrive(jnp.int32(0))
    load(jnp.int32(0))

    NT = N // T // 2

    def rows_of(base, n, size=T):
        return pl.ds(pl.multiple_of(base + n, LANES), size)

    NT2 = N // T

    def saved(i):
        return gsave_h.at[lax.div(i, NT2), :, tile(lax.rem(i, NT2), T), :]

    def save(i, go):
        sl = odd(i)
        cp = pltpu.make_async_copy(GST.at[sl], saved(i), g_sem.at[sl])
        cp.start() if go else cp.wait()

    def phase0(i, _):
        kk, t, sl = lax.div(i, NT2), lax.rem(i, NT2), odd(i)

        @pl.when(t == 0)
        def _():
            loaded(kk)

        @pl.when(t == 1)
        def _():
            gather_step(kk + 1)

        @pl.when(t == NT2 - 1)
        def _():
            arrive(kk + 1)
            load(kk + 1)

        @pl.when(i >= 2)
        def _():
            save(i - 2, False)
        w = odd(kk)
        for b in range(T // SUB):
            rows, k = rows_of(t * T, SUB * b, SUB), slice(SUB * b, SUB * b + SUB)
            a = A[rows, :]
            g, u = nn(a, WB[w, 0]), nn(a, WB[w, 1])
            GST[sl, 0, k] = g
            GST[sl, 1, k] = u
            p = (g / (1.0 + jnp.exp(-g)) * u).astype(bf16)
            ACC[rows, :] += nn(p, WB[w, 2])
        save(i, True)
        return 0

    lax.fori_loop(0, NC * NT2, phase0, 0)
    keep.wait()

    def between(t, _):
        r = tile(t, TB)
        h = (HB[r, :].astype(f32) + ACC[r, :].astype(bf16).astype(f32)).astype(bf16)
        HB[r, :] = h
        a = normed(h)
        A[r, :] = a
        AT[:, r] = a.T
        ACC[r, :] = jnp.zeros((TB, D), f32)
        return 0

    lax.fori_loop(0, N // TB, between, 0)
    save(jnp.int32(NC * NT2 - 2), False)
    save(jnp.int32(NC * NT2 - 1), False)
    gather_step(jnp.int32(NC + 1))

    def backward(kk, base, n_tiles, first, g, u, ahead, late):
        w, sl, per = odd(kk), odd(kk), T // SUB
        done = {}

        def rows(k):
            return rows_of(base, SUB * k, SUB)

        def block(k):
            g_b, u_b = g(rows(k), k), u(rows(k), k)
            by_p = nt(DY[rows(k), :], WB[w, 2]).astype(bf16).astype(f32)
            sig = 1.0 / (1.0 + jnp.exp(-g_b))
            act = g_b * sig
            done[k] = ((by_p * u_b * (sig + act * (1.0 - sig))).astype(bf16), (by_p * act).astype(bf16), (act * u_b).astype(bf16))

        def by_data(k):
            if late:
                A[rows(k), :] = done[k][0]
                HB[rows(k), :] = done[k][1]
            else:
                ACC[rows(k), :] += nt(done[k][0], WB[w, 0]) + nt(done[k][1], WB[w, 1])

        def by_weights(tile_n):
            for m, left in ((2, DYT),) if late else ((2, DYT), (1, AT), (0, AT)):
                term = nn(left[:, rows_of(base, T * tile_n)], jnp.concatenate([done[per * tile_n + k][m] for k in range(per)]))
                DW[sl, m] = (jnp.where(first, 0.0, DW[sl, m]) if tile_n == 0 else DW[sl, m]) + term

        blocks = n_tiles * per
        for k in range(ahead):
            block(k)
        for k in range(blocks):
            if k + ahead < blocks:
                block(k + ahead)
            by_data(k)
            if (k + 1) % per == 0:
                by_weights(k // per)

    def phase1(i, _):
        kk, t = NC + lax.div(i, NT), lax.rem(i, NT)

        @pl.when(t == 0)
        def _():
            loaded(kk)
            first_half(kk)

        @pl.when(t == 1)
        def _():
            @pl.when(kk + 1 < NM)
            def _():
                arrive(kk + 1)
            load(kk + 1)
            gather_step(kk + 2)
            second_half(kk)
        w = odd(kk)
        backward(kk, t * (2 * T), 2, t == 0, lambda rows, b: nn(A[rows, :], WB[w, 0]), lambda rows, b: nn(A[rows, :], WB[w, 1]), 0, False)
        return 0

    lax.fori_loop(0, NC * NT, phase1, 0)
    again = pltpu.make_async_copy(a0t_h, AT, io_sem.at[2])
    again.start()

    def fetch(i, go):
        sl = odd(i)
        cp = pltpu.make_async_copy(saved(i), GST.at[sl], g_sem.at[sl])
        cp.start() if go else cp.wait()

    fetch(jnp.int32(0), True)

    def turn(t, _):
        r = tile(t, TB)
        by_a = ACC[r, :].astype(bf16).astype(f32)
        by_h = (DY[r, :].astype(f32) + through_norm(by_a, HB[r, :]).astype(bf16).astype(f32)).astype(bf16)
        DY[r, :] = by_h
        DYT[:, r] = by_h.T
        ACC[r, :] = jnp.zeros((TB, D), f32)
        return 0

    lax.fori_loop(0, N // TB, turn, 0)
    again.wait()

    def xtile(t, go):
        k = lax.rem(t, 3)
        cp = pltpu.make_async_copy(x_h.at[tile(t, TB)], WB.at[0, k], x_sem.at[k])
        cp.start() if go else cp.wait()

    end = jnp.int32(NM - 1)

    def backward_tile(i, late):
        kk, t, sl = 2 * NC + lax.div(i, NT2), lax.rem(i, NT2), odd(i)

        @pl.when(t == 0)
        def _():
            loaded(kk)
            first_half(kk)

        @pl.when(t == 1)
        def _():
            second_half(kk)

        if late:
            @pl.when(t == NT2 - 1)
            def _():
                last_gu(end - 2, 0)
                plane_gu(end - 1, 0)

        @pl.when(t == NT2 - 1)
        def _():
            if late:
                for k in range(3):
                    xtile(jnp.int32(k), True)
            else:
                load(kk + 1)

        @pl.when(i + 1 < NC * NT2)
        def _():
            fetch(i + 1, True)
        fetch(i, False)
        backward(kk, t * T, 1, t == 0, lambda rows, b: GST[sl, 0, SUB * b:SUB * b + SUB], lambda rows, b: GST[sl, 1, SUB * b:SUB * b + SUB], 1, late)
        return 0

    lax.fori_loop(0, (NC - 1) * NT2, lambda i, _: backward_tile(i, False), 0)
    lax.fori_loop((NC - 1) * NT2, NC * NT2, lambda i, _: backward_tile(i, True), 0)
    def finish(t, _):
        xtile(t, False)
        r = tile(t, TB)
        by_a = (ACC[r, :] + nt(A[r, :], WB[1, 0]) + nt(HB[r, :], WB[1, 1])).astype(bf16).astype(f32)
        DY[r, :] = (DY[r, :].astype(f32) + through_norm(by_a, WB[0, lax.rem(t, 3)]).astype(bf16).astype(f32)).astype(bf16)

        @pl.when(t + 3 < N // TB)
        def _():
            xtile(t + 3, True)
        return 0


    def finish_some(first, many):
        lax.fori_loop(first * N // TB // 8, (first + many) * N // TB // 8, finish, 0)

    pair_send_d(end)
    last_gu(end - 2, 1)
    last_d(end - 2)
    DW[1, 0] = nn(AT[...], A[...])
    pair_send_gu(end, 0)
    plane_gu(end - 1, 1)
    pair_sum_d(end)
    last_gu(end - 1, 0)
    DW[1, 1] = nn(AT[...], HB[...])
    pair_send_gu(end, 1)
    plane_d(end - 1)
    pair_sum_gu(end, 0)
    finish_some(0, 2)
    pair_sum_gu(end, 1)
    last_gu(end - 1, 1)
    finish_some(2, 2)
    plane_d(end)
    last_d(end - 1)
    finish_some(4, 1)
    plane_gu(end, 0)
    finish_some(5, 2)
    plane_gu(end, 1)
    last_d(end)
    finish_some(7, 1)
    last_gu(end, 0)
    pltpu.make_async_copy(DY, dx_h, io_sem.at[1]).start()
    last_gu(end, 1)

    def settle(kk, _):
        sent_all(kk)
        return 0

    lax.fori_loop(0, NM, settle, 0)
    for m in (end - 1, end):
        for n in range(2):
            ended_gu(m, n)
        ended_d(m)
    for n in range(2):
        wait_for(S1GU.at[n], rs.at[PAIR_OUT, n, 1])
        wait_for(R2GU.at[0, n], rs.at[PLANE_OUT, n, 1])
        wait_for(R3GU.at[0, n], rs.at[ACROSS_OUT, n, 1])
        wait_for(S3GU.at[n], rs.at[ROUND_OUT, n, 1])

    def sent_d(m):
        sl = m % 2
        wait_for(R2D, rs.at[PLANE_OUT, DOWN, sl])
        wait_for(R3D, rs.at[ACROSS_OUT, DOWN, sl])
        wait_for(S3D, rs.at[ROUND_OUT, DOWN, sl])

    @pl.when(e == 0)
    def _():
        wait_for(S1D, rs.at[PAIR_OUT, DOWN, 1])
        sent_d(NM - 2)

    @pl.when(e == 1)
    def _():
        wait_for(S1D, rs.at[PAIR_OUT, DOWN, 0])
        sent_d(NM - 1)
    wait_for(DY, io_sem.at[1])


def deliver(dx_i, gu_i, d_i, dx_o, g_o, u_o, d_o, DX, GU, DN, OG, OU, OD, sem_in, sem_out):
    parts = 4
    n = DX.shape[0] // parts
    moves = [(gu_i, GU), (d_i, DN)] + [(dx_i.at[pl.ds(n * i, n)], DX.at[pl.ds(n * i, n)]) for i in range(parts)]
    ins = [pltpu.make_async_copy(src, dst, sem_in.at[i]) for i, (src, dst) in enumerate(moves)]
    outs = [pltpu.make_async_copy(src, dst, sem_out.at[i]) for i, (src, dst) in enumerate(
        [(DX.at[pl.ds(n * i, n)], dx_o.at[pl.ds(n * i, n)]) for i in range(parts)] + [(OG, g_o), (OU, u_o), (OD, d_o)])]
    for cp in ins:
        cp.start()
    ins[0].wait()
    for l in range(LAYERS):
        for c in range(NC):
            for p in range(4):
                at = 384 * (2 * p + c % 2) + LANES * (c // 2)
                for y in range(Z):
                    OG[l, QUARTER * y:QUARTER * y + QUARTER, at:at + LANES] = GU[l, c, y, 0, :, LANES * p:LANES * p + LANES]
                    OU[l, QUARTER * y:QUARTER * y + QUARTER, at:at + LANES] = GU[l, c, y, 1, :, LANES * p:LANES * p + LANES]
    outs[parts].start()
    outs[parts + 1].start()
    ins[1].wait()
    for l in range(LAYERS):
        for j in range(3):
            for y in range(Z):
                OD[l, LANES * j:LANES * j + LANES, LANES * y:LANES * y + LANES] = DN[l, j, y].T
    outs[parts + 2].start()
    for i in range(parts):
        ins[2 + i].wait()
        outs[i].start()
    for cp in outs:
        cp.wait()


def solution(mesh, T=1024, TB=D):
    def step(x, dy, w_gate, w_up, w_down):
        N = x.shape[1]
        hbm = pl.BlockSpec(memory_space=pl.ANY)
        sds = jax.ShapeDtypeStruct
        v, dma = pltpu.VMEM, pltpu.SemaphoreType.DMA
        dx, ogu, od, *_ = pl.pallas_call(
            functools.partial(kernel, T, TB),
            name="step",
            out_shape=[
                sds((N, D), bf16), sds((LAYERS, NC, Z, 2, QUARTER, F), bf16), sds((LAYERS, 3, Z, LANES, LANES), bf16),
                sds((LAYERS, NC, 2, D, F), bf16), sds((LAYERS, NC, 4, Z, 32, D), bf16), sds((NC, 2, N, F), f32), sds((D, N), bf16),
            ],
            in_specs=[hbm] * 5,
            out_specs=[hbm] * 7,
            scratch_shapes=[
                v((N, D), bf16), v((D, N), bf16), v((N, D), bf16), v((D, N), bf16), v((N, D), bf16), v((N, D), f32),
                v((2, 3, D, D), bf16), v((2, 3, D, D), f32), v((2, 2, T, F), f32), v((NC, 2, ROWS, F), bf16),
                v((2, 4, ROWS, F), bf16), v((4, D, LANES), bf16), v((2, 2, 4, ROWS, F), bf16), v((4, D, LANES), bf16),
                v((2, 4, ROWS, F), bf16), v((4, D, LANES), bf16), v((2, ROWS, F), f32), v((D, LANES), f32), v((2, 2, 3, ROWS, F), bf16), v((3, D, LANES), bf16),
                v((2, 4, QUARTER, F), bf16), v((4, LANES, LANES), bf16), v((2, QUARTER, F), f32), v((LANES, LANES), f32), v((2, 2, 3, QUARTER, F), bf16), v((3, LANES, LANES), bf16),
                v((2, QUARTER, F), bf16), v((LANES, LANES), bf16),
                dma((NM,)), dma((3,)), dma((2,)), dma((2,)), *[dma((NM,)) for _ in range(7)], dma((3,)), dma((8, 3, 2)),
            ],
            compiler_params=pltpu.CompilerParams(collective_id=0, has_side_effects=True, vmem_limit_bytes=67043328),
        )(x[0], dy[0], w_gate, w_up, w_down)
        dx, *by_w = pl.pallas_call(
            deliver,
            name="deliver",
            out_shape=[sds((N, D), bf16), sds((LAYERS, ROWS, FF), bf16), sds((LAYERS, ROWS, FF), bf16), sds((LAYERS, 384, D), bf16)],
            in_specs=[hbm] * 3,
            out_specs=[hbm] * 4,
            scratch_shapes=[
                v((N, D), bf16), v((LAYERS, NC, Z, 2, QUARTER, F), bf16), v((LAYERS, 3, Z, LANES, LANES), bf16),
                v((LAYERS, ROWS, FF), bf16), v((LAYERS, ROWS, FF), bf16), v((LAYERS, 384, D), bf16), dma((6,)), dma((7,)),
            ],
            compiler_params=pltpu.CompilerParams(vmem_limit_bytes=67043328),
        )(dx, ogu, od)
        return dx[None], *by_w

    states, cut = P(("rep", "r", "s"), None, None), P(None, "s", None)
    return jax.shard_map(
        step,
        mesh=mesh,
        in_specs=(states, states) + (cut,) * 3,
        out_specs=(states,) + (P("rep", "s", None),) * 3,
        check_vma=False,
    )
```

```python
import functools

import jax
import jax.numpy as jnp
from jax import lax
from jax.experimental import pallas as pl
from jax.experimental.pallas import tpu as pltpu
from jax.sharding import PartitionSpec as P

MESH = pl.DeviceIdType.MESH
DOWN = 2
LANES, ROWS, QUARTER = 128, 64, 16
PAIR_OUT, PAIR_IN, PLANE_OUT, PLANE_IN, ACROSS_OUT, ACROSS_IN, ROUND_OUT, ROUND_IN = range(8)
f32, bf16 = jnp.float32, jnp.bfloat16
D, FF, F, NC, LAYERS, S, Z = 512, 3072, 512, 6, 2, 8, 4
SUB = 512
NM = NC * LAYERS


def odd(n):
    return lax.rem(n, 2)


def nn(a, b):
    return jnp.dot(a, b, preferred_element_type=f32)


def nt(a, b):
    return lax.dot_general(a, b, (((1,), (1,)), ((), ())), preferred_element_type=f32)


def normed(h):
    wide = h.astype(f32)
    return (wide * lax.rsqrt(jnp.mean(wide * wide, -1, keepdims=True) + 1e-6)).astype(bf16)


def through_norm(by_a, h):
    wide = h.astype(f32)
    scale = lax.rsqrt(jnp.mean(wide * wide, -1, keepdims=True) + 1e-6)
    along = jnp.mean(by_a * wide, -1, keepdims=True)
    return by_a * scale - wide * (scale * scale * scale * along)


def wait_for(ref, sem):
    pltpu.make_async_copy(ref, ref, sem).wait()


def kernel(T, TB, x_h, dy_h, wg_h, wu_h, wd_h,
           dx_h, ogu_h, od_h, wgu_f, wd_f, gsave_h, a0t_h,
           A, AT, DY, DYT, HB, ACC, WB, DW, GST, SGU,
           S1GU, S1D, R1GU, R1D, S2GU, S2D, P2GU, P2D, R2GU, R2D,
           S3GU, S3D, P3GU, P3D, R3GU, R3D, S4GU, S4D,
           st_sem, io_sem, wl_sem, g_sem, gi, di, dz, gd, dd, ags, ads, x_sem, rs):
    N = A.shape[0]
    s, z = lax.axis_index("s"), lax.axis_index("r")
    e, q = odd(s), lax.div(s, 2)
    qx, qy = lax.div(q, 2), odd(q)
    others = (2 * (1 - qx) + qy, 2 * qx + 1 - qy, 2 * (1 - qx) + 1 - qy)
    partner = {"s": 2 * q + 1 - e}

    def chip(i):
        return {"s": 2 * others[i] + e}

    def plane(i):
        return lax.rem(z + i, Z)

    def remote(src, dst, send, recv, to):
        pltpu.make_async_remote_copy(src_ref=src, dst_ref=dst, send_sem=send, recv_sem=recv, device_id=to, device_id_type=MESH).start()

    def split(kk):
        l = lax.div(kk, NC)
        c = lax.rem(kk, NC)
        return l, c, odd(c), lax.div(c, 2)

    def own_gu(kk):
        l, c, h, j = split(kk)
        wait_for(SGU.at[c], st_sem.at[kk])
        src, dst = SGU.at[c], wgu_f.at[l, c, :, pl.ds(pl.multiple_of(ROWS * s, ROWS), ROWS), :]
        for i in range(3):
            remote(src, dst, ags.at[kk], gi.at[kk], chip(i))
        remote(src, dst, ags.at[kk], gd.at[kk], partner)
        pltpu.make_async_copy(src, dst, gi.at[kk]).start()

    def forward_gu(kk):
        l, c, h, j = split(kk)
        wait_for(wgu_f.at[l, c, :, pl.ds(0, 256), :], gi.at[kk])
        for i in range(3):
            block = wgu_f.at[l, c, :, pl.ds(pl.multiple_of(ROWS * (2 * others[i] + e), ROWS), ROWS), :]
            remote(block, block, ags.at[kk], gd.at[kk], partner)

    def when_mine(kk, do):
        l, c, h, j = split(kk)

        @pl.when(h == e)
        def _():
            do(l, c, j)

    def own_d(kk):
        def do(l, c, j):
            src, dst = wd_h.at[l, pl.ds(pl.multiple_of(LANES * j + ROWS * odd(z), ROWS), ROWS), :], wd_f.at[l, c, q, odd(z)]
            for i in range(3):
                remote(src, dst, ads.at[kk], di.at[kk], chip(i))
            pltpu.make_async_copy(src, dst, di.at[kk]).start()
        when_mine(kk, do)

    def across_d(kk):
        def do(l, c, j):
            block = wd_f.at[l, c, :, odd(z)]
            wait_for(block, di.at[kk])
            remote(block, block, ads.at[kk], dz.at[kk], {"r": z + 1 - 2 * odd(z)})
        when_mine(kk, do)

    def forward_d(kk):
        def do(l, c, j):
            wait_for(wd_f.at[l, c, :, 0], dz.at[kk])
            remote(wd_f.at[l, c], wd_f.at[l, c], ads.at[kk], dd.at[kk], partner)
        when_mine(kk, do)

    def arrive_gu(kk):
        l, c, h, j = split(kk)
        wait_for(wgu_f.at[l, c, :, pl.ds(0, 256), :], gd.at[kk])

    def arrive_d(kk):
        l, c, h, j = split(kk)

        @pl.when(h != e)
        def _():
            wait_for(wd_f.at[l, c], dd.at[kk])

    def arrive(kk):
        arrive_gu(kk)
        arrive_d(kk)

    def stage(kk, _):
        l, c, h, j = split(kk)
        for p in range(4):
            cols = pl.ds(pl.multiple_of(384 * (2 * p + h) + LANES * j, LANES), LANES)
            for n, w in enumerate((wg_h, wu_h)):
                pltpu.make_async_copy(w.at[l, :, cols], SGU.at[c, n, :, pl.ds(LANES * p, LANES)], st_sem.at[kk]).start()
        return 0

    def gather_step(k):
        def go(do, kk):
            @pl.when(kk < NM)
            def _():
                do(kk)
        go(forward_gu, k)
        go(forward_d, k)

        @pl.when(jnp.logical_and(k >= NC - 3, k + 3 < NM))
        def _():
            wait_for(wgu_f.at[0, 0, :, pl.ds(0, 448), :], ags.at[k + 3 - NC])
            stage(k + 3, 0)
        go(across_d, k + 2)
        go(own_d, k + 3)
        go(own_gu, k + 2)

    def load_gu(kk):
        l, c, slot = odd(lax.div(kk, NC)), lax.rem(kk, NC), odd(kk)
        pltpu.make_async_copy(wgu_f.at[l, c], WB.at[slot, pl.ds(0, DOWN)], wl_sem.at[slot]).start()

    def load_d(kk):
        l, c, slot = odd(lax.div(kk, NC)), lax.rem(kk, NC), odd(kk)
        for p in range(4):
            for y in range(2):
                pltpu.make_async_copy(wd_f.at[l, c, p, y], WB.at[slot, DOWN, pl.ds(LANES * p + ROWS * y, ROWS)], wl_sem.at[slot]).start()

    def load(kk):
        load_gu(kk)
        load_d(kk)

    def loaded(kk):
        slot = odd(kk)
        wait_for(WB.at[slot], wl_sem.at[slot])

    def sent_all(kk):
        l, c, h, j = split(kk)
        @pl.when(kk >= NC)
        def _():
            wait_for(wgu_f.at[l, c, :, pl.ds(0, 448), :], ags.at[kk])

        @pl.when(h == e)
        def _():
            wait_for(wgu_f.at[l, c, :, pl.ds(0, 480), :], ads.at[kk])

    def place(m):
        l = 1 - lax.div(m, NC)
        c = lax.rem(m, NC)
        return l, c, odd(c), lax.div(c, 2), odd(m)

    def rows64(block):
        return pl.ds(pl.multiple_of(ROWS * block, ROWS), ROWS)

    def pair_send_gu(m, n):
        sl = odd(m)

        @pl.when(m >= 1)
        def _():
            wait_for(S1GU.at[n], rs.at[PAIR_OUT, n, 1 - sl])
        for p in range(4):
            S1GU[n, p] = DW[sl, n, rows64(2 * p + 1 - e), :].astype(bf16)
        remote(S1GU.at[n], R1GU.at[sl, n], rs.at[PAIR_OUT, n, sl], rs.at[PAIR_IN, n, sl], partner)

    def pair_send_d(m):
        l, c, h, j, sl = place(m)

        @pl.when(h != e)
        def _():
            @pl.when(m >= 2)
            def _():
                wait_for(S1D, rs.at[PAIR_OUT, DOWN, sl])
            for p in range(4):
                S1D[p] = DW[sl, 2, :, LANES * p:LANES * p + LANES].astype(bf16)
            remote(S1D, R1D, rs.at[PAIR_OUT, DOWN, sl], rs.at[PAIR_IN, DOWN, sl], partner)

    def pair_sum_gu(m, n):
        sl = odd(m)
        wait_for(R1GU.at[sl, n], rs.at[PAIR_IN, n, sl])

        @pl.when(m >= 1)
        def _():
            wait_for(R2GU.at[0, n], rs.at[PLANE_OUT, n, 1 - sl])
        for p in range(4):
            S2GU[n, p] = (DW[sl, n, rows64(2 * p + e), :] + R1GU[sl, n, p].astype(f32)).astype(bf16)
        P2GU[n] = DW[sl, n, rows64(2 * q + e), :] + R1GU[sl, n, q].astype(f32)
        for i in range(3):
            remote(S2GU.at[n, others[i]], R2GU.at[sl, n, i], rs.at[PLANE_OUT, n, sl], rs.at[PLANE_IN, n, sl], chip(i))

    def pair_sum_d(m):
        l, c, h, j, sl = place(m)

        @pl.when(h == e)
        def _():
            wait_for(R1D, rs.at[PAIR_IN, DOWN, sl])

            @pl.when(m >= 2)
            def _():
                wait_for(R2D, rs.at[PLANE_OUT, DOWN, sl])
            for p in range(4):
                total = DW[sl, 2, :, LANES * p:LANES * p + LANES] + R1D[p].astype(f32)
                S2D[p] = total.astype(bf16)

                @pl.when(q == p)
                def _():
                    P2D[...] = total
            for i in range(3):
                remote(S2D.at[others[i]], R2D.at[i], rs.at[PLANE_OUT, DOWN, sl], rs.at[PLANE_IN, DOWN, sl], chip(i))

    def ended_gu(m, n):
        wait_for(R3GU.at[0, n], rs.at[ROUND_IN, n, odd(m)])

    def ended_d(m):
        l, c, h, j, sl = place(m)

        @pl.when(h == e)
        def _():
            wait_for(R3D, rs.at[ROUND_IN, DOWN, sl])

    def plane_gu(m, n):
        sl = odd(m)
        wait_for(R2GU.at[sl, n], rs.at[PLANE_IN, n, sl])

        @pl.when(m >= 1)
        def _():
            wait_for(R3GU.at[0, n], rs.at[ACROSS_OUT, n, 1 - sl])

        @pl.when(m >= 2)
        def _():
            ended_gu(m - 2, n)
        for p in range(4):
            k = slice(QUARTER * p, QUARTER * p + QUARTER)
            total = P2GU[n, k, :]
            for i in range(3):
                total += R2GU[sl, n, i, k, :].astype(f32)
            S3GU[n, p] = total.astype(bf16)

            @pl.when(z == p)
            def _():
                P3GU[n] = total
        for i in range(1, 4):
            remote(S3GU.at[n, plane(i)], R3GU.at[sl, n, i - 1], rs.at[ACROSS_OUT, n, sl], rs.at[ACROSS_IN, n, sl], {"r": plane(i)})

    def plane_d(m):
        l, c, h, j, sl = place(m)

        @pl.when(h == e)
        def _():
            wait_for(R2D, rs.at[PLANE_IN, DOWN, sl])

            @pl.when(m >= 2)
            def _():
                wait_for(R3D, rs.at[ACROSS_OUT, DOWN, sl])
                ended_d(m - 2)
            for p in range(4):
                k = slice(LANES * p, LANES * p + LANES)
                total = P2D[k, :]
                for i in range(3):
                    total += R2D[i, k, :].astype(f32)
                S3D[p] = total.astype(bf16)

                @pl.when(z == p)
                def _():
                    P3D[...] = total
            for i in range(1, 4):
                remote(S3D.at[plane(i)], R3D.at[i - 1], rs.at[ACROSS_OUT, DOWN, sl], rs.at[ACROSS_IN, DOWN, sl], {"r": plane(i)})

    def last_gu(m, n):
        l, c, h, j, sl = place(m)
        wait_for(R3GU.at[sl, n], rs.at[ACROSS_IN, n, sl])

        @pl.when(m >= 1)
        def _():
            wait_for(S3GU.at[n], rs.at[ROUND_OUT, n, 1 - sl])
        S4GU[n] = (P3GU[n] + R3GU[sl, n, 0].astype(f32) + R3GU[sl, n, 1].astype(f32) + R3GU[sl, n, 2].astype(f32)).astype(bf16)
        dst = ogu_h.at[l, c, z, n]
        for i in range(1, 4):
            remote(S4GU.at[n], dst, rs.at[ROUND_OUT, n, sl], rs.at[ROUND_IN, n, sl], {"r": plane(i)})
        pltpu.make_async_copy(S4GU.at[n], dst, rs.at[ROUND_OUT, n, sl]).start()

    def last_d(m):
        l, c, h, j, sl = place(m)

        @pl.when(h == e)
        def _():
            wait_for(R3D, rs.at[ACROSS_IN, DOWN, sl])

            @pl.when(m >= 2)
            def _():
                wait_for(S3D, rs.at[ROUND_OUT, DOWN, sl])
            S4D[...] = (P3D[...] + R3D[0].astype(f32) + R3D[1].astype(f32) + R3D[2].astype(f32)).astype(bf16)
            dst = od_h.at[l, j, z]
            for i in range(1, 4):
                remote(S4D, dst, rs.at[ROUND_OUT, DOWN, sl], rs.at[ROUND_IN, DOWN, sl], {"r": plane(i)})
            pltpu.make_async_copy(S4D, dst, rs.at[ROUND_OUT, DOWN, sl]).start()

    def whole(gu, d, m):
        gu(m, 0)
        gu(m, 1)
        d(m)

    def pair_send(m):
        whole(pair_send_gu, pair_send_d, m)

    def pair_sum(m):
        whole(pair_sum_gu, pair_sum_d, m)

    def plane_sum(m):
        whole(plane_gu, plane_d, m)

    def last_sum(m):
        whole(last_gu, last_d, m)

    def first_half(kk):
        @pl.when(kk >= NC + 3)
        def _():
            last_sum(kk - NC - 3)

        @pl.when(kk >= NC + 1)
        def _():
            pair_send(kk - NC - 1)

    def second_half(kk):
        @pl.when(kk >= NC + 2)
        def _():
            plane_sum(kk - NC - 2)

        @pl.when(kk >= NC + 1)
        def _():
            pair_sum(kk - NC - 1)

    def tile(t, T):
        return pl.ds(pl.multiple_of(t * T, T), T)

    xin = pltpu.make_async_copy(x_h, HB, io_sem.at[0])
    dyin = pltpu.make_async_copy(dy_h, DY, io_sem.at[1])
    barrier = pltpu.get_barrier_semaphore()
    peers = [partner] + [chip(i) for i in range(3)] + [{"r": plane(i)} for i in range(1, 4)]
    for to in peers:
        pl.semaphore_signal(barrier, 1, device_id=to, device_id_type=MESH)
    stage(jnp.int32(0), 0)
    pl.semaphore_wait(barrier, len(peers))
    own_d(jnp.int32(0))
    own_gu(jnp.int32(0))
    own_d(jnp.int32(1))
    own_d(jnp.int32(2))
    xin.start()
    dyin.start()
    lax.fori_loop(1, NC, stage, 0)
    xin.wait()
    dyin.wait()

    def prepare(t, _):
        r = tile(t, TB)
        a = normed(HB[r, :])
        A[r, :] = a
        AT[:, r] = a.T
        DYT[:, r] = DY[r, :].T
        return 0

    across_d(jnp.int32(0))
    lax.fori_loop(0, N // TB, prepare, 0)
    keep = pltpu.make_async_copy(AT, a0t_h, io_sem.at[2])
    keep.start()
    across_d(jnp.int32(1))
    forward_gu(jnp.int32(0))
    own_d(jnp.int32(3))
    own_gu(jnp.int32(1))
    arrive_gu(jnp.int32(0))
    load_gu(jnp.int32(0))

    NT = N // T // 2

    def rows_of(base, n, size=T):
        return pl.ds(pl.multiple_of(base + n, LANES), size)

    NT2 = N // T

    def saved(i):
        return gsave_h.at[lax.div(i, NT2), :, tile(lax.rem(i, NT2), T), :]

    def save(i, go):
        sl = odd(i)
        cp = pltpu.make_async_copy(GST.at[sl], saved(i), g_sem.at[sl])
        cp.start() if go else cp.wait()

    def phase0(i, _):
        kk, t, sl = lax.div(i, NT2), lax.rem(i, NT2), odd(i)

        @pl.when(t == 0)
        def _():
            loaded(kk)

        @pl.when(t == 1)
        def _():
            gather_step(kk + 1)

        @pl.when(t == NT2 - 1)
        def _():
            arrive(kk + 1)
            load(kk + 1)

        @pl.when(i >= 2)
        def _():
            save(i - 2, False)
        w = odd(kk)
        for b in range(T // SUB):
            rows, k = rows_of(t * T, SUB * b, SUB), slice(SUB * b, SUB * b + SUB)
            a = A[rows, :]
            g, u = nn(a, WB[w, 0]), nn(a, WB[w, 1])
            GST[sl, 0, k] = g
            GST[sl, 1, k] = u
            p = (g / (1.0 + jnp.exp(-g)) * u).astype(bf16)
            ACC[rows, :] += nn(p, WB[w, 2])
        save(i, True)
        return 0

    def first_gate(t, _):
        sl = odd(t)

        @pl.when(t == 1)
        def _():
            forward_d(jnp.int32(0))
            across_d(jnp.int32(2))
            own_gu(jnp.int32(2))

        @pl.when(t == NT2 - 1)
        def _():
            arrive_d(jnp.int32(0))
            load_d(jnp.int32(0))

        @pl.when(t >= 2)
        def _():
            save(t - 2, False)
        for b in range(T // SUB):
            rows, k = rows_of(t * T, SUB * b, SUB), slice(SUB * b, SUB * b + SUB)
            a = A[rows, :]
            g, u = nn(a, WB[0, 0]), nn(a, WB[0, 1])
            GST[sl, 0, k] = g
            GST[sl, 1, k] = u
            ACC[rows, :] = g / (1.0 + jnp.exp(-g)) * u
        save(t, True)
        return 0

    def first_down(t, _):
        @pl.when(t == 0)
        def _():
            gather_step(jnp.int32(1))

        @pl.when(t == NT2 - 1)
        def _():
            arrive(jnp.int32(1))
            load(jnp.int32(1))
        for b in range(T // SUB):
            rows = rows_of(t * T, SUB * b, SUB)
            ACC[rows, :] = nn(ACC[rows, :].astype(bf16), WB[0, DOWN])
        return 0

    wait_for(WB.at[0, pl.ds(0, DOWN)], wl_sem.at[0])
    lax.fori_loop(0, NT2, first_gate, 0)
    wait_for(WB.at[0, DOWN], wl_sem.at[0])
    lax.fori_loop(0, NT2, first_down, 0)
    lax.fori_loop(NT2, NC * NT2, phase0, 0)
    keep.wait()

    def between(t, _):
        r = tile(t, TB)
        h = (HB[r, :].astype(f32) + ACC[r, :].astype(bf16).astype(f32)).astype(bf16)
        HB[r, :] = h
        a = normed(h)
        A[r, :] = a
        AT[:, r] = a.T
        ACC[r, :] = jnp.zeros((TB, D), f32)
        return 0

    lax.fori_loop(0, N // TB, between, 0)
    save(jnp.int32(NC * NT2 - 2), False)
    save(jnp.int32(NC * NT2 - 1), False)
    gather_step(jnp.int32(NC + 1))

    def backward(kk, base, n_tiles, first, g, u, ahead, late):
        w, sl, per = odd(kk), odd(kk), T // SUB
        done = {}

        def rows(k):
            return rows_of(base, SUB * k, SUB)

        def block(k):
            g_b, u_b = g(rows(k), k), u(rows(k), k)
            by_p = nt(DY[rows(k), :], WB[w, 2]).astype(bf16).astype(f32)
            sig = 1.0 / (1.0 + jnp.exp(-g_b))
            act = g_b * sig
            done[k] = ((by_p * u_b * (sig + act * (1.0 - sig))).astype(bf16), (by_p * act).astype(bf16), (act * u_b).astype(bf16))

        def by_data(k):
            if late:
                A[rows(k), :] = done[k][0]
                HB[rows(k), :] = done[k][1]
            else:
                ACC[rows(k), :] += nt(done[k][0], WB[w, 0]) + nt(done[k][1], WB[w, 1])

        def by_weights(tile_n):
            for m, left in ((2, DYT),) if late else ((2, DYT), (1, AT), (0, AT)):
                term = nn(left[:, rows_of(base, T * tile_n)], jnp.concatenate([done[per * tile_n + k][m] for k in range(per)]))
                DW[sl, m] = (jnp.where(first, 0.0, DW[sl, m]) if tile_n == 0 else DW[sl, m]) + term

        blocks = n_tiles * per
        for k in range(ahead):
            block(k)
        for k in range(blocks):
            if k + ahead < blocks:
                block(k + ahead)
            by_data(k)
            if (k + 1) % per == 0:
                by_weights(k // per)

    def phase1(i, _):
        kk, t = NC + lax.div(i, NT), lax.rem(i, NT)

        @pl.when(t == 0)
        def _():
            loaded(kk)
            first_half(kk)

        @pl.when(t == 1)
        def _():
            @pl.when(kk + 1 < NM)
            def _():
                arrive(kk + 1)
            load(kk + 1)
            gather_step(kk + 2)
            second_half(kk)
        w = odd(kk)
        backward(kk, t * (2 * T), 2, t == 0, lambda rows, b: nn(A[rows, :], WB[w, 0]), lambda rows, b: nn(A[rows, :], WB[w, 1]), 0, False)
        return 0

    lax.fori_loop(0, NC * NT, phase1, 0)
    again = pltpu.make_async_copy(a0t_h, AT, io_sem.at[2])
    again.start()

    def fetch(i, go):
        sl = odd(i)
        cp = pltpu.make_async_copy(saved(i), GST.at[sl], g_sem.at[sl])
        cp.start() if go else cp.wait()

    fetch(jnp.int32(0), True)

    def turn(t, _):
        r = tile(t, TB)
        by_a = ACC[r, :].astype(bf16).astype(f32)
        by_h = (DY[r, :].astype(f32) + through_norm(by_a, HB[r, :]).astype(bf16).astype(f32)).astype(bf16)
        DY[r, :] = by_h
        DYT[:, r] = by_h.T
        ACC[r, :] = jnp.zeros((TB, D), f32)
        return 0

    lax.fori_loop(0, N // TB, turn, 0)
    again.wait()

    def xtile(t, go):
        k = lax.rem(t, 3)
        cp = pltpu.make_async_copy(x_h.at[tile(t, TB)], WB.at[0, k], x_sem.at[k])
        cp.start() if go else cp.wait()

    end = jnp.int32(NM - 1)

    def backward_tile(i, late):
        kk, t, sl = 2 * NC + lax.div(i, NT2), lax.rem(i, NT2), odd(i)

        @pl.when(t == 0)
        def _():
            loaded(kk)
            first_half(kk)

        @pl.when(t == 1)
        def _():
            second_half(kk)

        if late:
            @pl.when(t == NT2 - 1)
            def _():
                last_gu(end - 2, 0)
                plane_gu(end - 1, 0)

        @pl.when(t == NT2 - 1)
        def _():
            if late:
                for k in range(3):
                    xtile(jnp.int32(k), True)
            else:
                load(kk + 1)

        @pl.when(i + 1 < NC * NT2)
        def _():
            fetch(i + 1, True)
        fetch(i, False)
        backward(kk, t * T, 1, t == 0, lambda rows, b: GST[sl, 0, SUB * b:SUB * b + SUB], lambda rows, b: GST[sl, 1, SUB * b:SUB * b + SUB], 1, late)
        return 0

    lax.fori_loop(0, (NC - 1) * NT2, lambda i, _: backward_tile(i, False), 0)
    lax.fori_loop((NC - 1) * NT2, NC * NT2, lambda i, _: backward_tile(i, True), 0)
    def finish(t, _):
        xtile(t, False)
        r = tile(t, TB)
        by_a = (ACC[r, :] + nt(A[r, :], WB[1, 0]) + nt(HB[r, :], WB[1, 1])).astype(bf16).astype(f32)
        DY[r, :] = (DY[r, :].astype(f32) + through_norm(by_a, WB[0, lax.rem(t, 3)]).astype(bf16).astype(f32)).astype(bf16)

        @pl.when(t + 3 < N // TB)
        def _():
            xtile(t + 3, True)
        return 0


    def finish_some(first, many):
        lax.fori_loop(first * N // TB // 8, (first + many) * N // TB // 8, finish, 0)

    pair_send_d(end)
    last_gu(end - 2, 1)
    last_d(end - 2)
    DW[1, 0] = nn(AT[...], A[...])
    pair_send_gu(end, 0)
    plane_gu(end - 1, 1)
    pair_sum_d(end)
    last_gu(end - 1, 0)
    DW[1, 1] = nn(AT[...], HB[...])
    pair_send_gu(end, 1)
    plane_d(end - 1)
    pair_sum_gu(end, 0)
    finish_some(0, 2)
    pair_sum_gu(end, 1)
    last_gu(end - 1, 1)
    finish_some(2, 2)
    plane_d(end)
    last_d(end - 1)
    finish_some(4, 1)
    plane_gu(end, 0)
    finish_some(5, 2)
    plane_gu(end, 1)
    last_d(end)
    finish_some(7, 1)
    last_gu(end, 0)
    pltpu.make_async_copy(DY, dx_h, io_sem.at[1]).start()
    last_gu(end, 1)

    def settle(kk, _):
        sent_all(kk)
        return 0

    lax.fori_loop(0, NM, settle, 0)
    for m in (end - 1, end):
        for n in range(2):
            ended_gu(m, n)
        ended_d(m)
    for n in range(2):
        wait_for(S1GU.at[n], rs.at[PAIR_OUT, n, 1])
        wait_for(R2GU.at[0, n], rs.at[PLANE_OUT, n, 1])
        wait_for(R3GU.at[0, n], rs.at[ACROSS_OUT, n, 1])
        wait_for(S3GU.at[n], rs.at[ROUND_OUT, n, 1])

    def sent_d(m):
        sl = m % 2
        wait_for(R2D, rs.at[PLANE_OUT, DOWN, sl])
        wait_for(R3D, rs.at[ACROSS_OUT, DOWN, sl])
        wait_for(S3D, rs.at[ROUND_OUT, DOWN, sl])

    @pl.when(e == 0)
    def _():
        wait_for(S1D, rs.at[PAIR_OUT, DOWN, 1])
        sent_d(NM - 2)

    @pl.when(e == 1)
    def _():
        wait_for(S1D, rs.at[PAIR_OUT, DOWN, 0])
        sent_d(NM - 1)
    wait_for(DY, io_sem.at[1])


def deliver(dx_i, gu_i, d_i, dx_o, g_o, u_o, d_o, DX, GU, DN, OG, OU, OD, sem_in, sem_out):
    parts = 4
    n = DX.shape[0] // parts
    moves = [(gu_i, GU), (d_i, DN)] + [(dx_i.at[pl.ds(n * i, n)], DX.at[pl.ds(n * i, n)]) for i in range(parts)]
    ins = [pltpu.make_async_copy(src, dst, sem_in.at[i]) for i, (src, dst) in enumerate(moves)]
    outs = [pltpu.make_async_copy(src, dst, sem_out.at[i]) for i, (src, dst) in enumerate(
        [(DX.at[pl.ds(n * i, n)], dx_o.at[pl.ds(n * i, n)]) for i in range(parts)] + [(OG, g_o), (OU, u_o), (OD, d_o)])]
    for cp in ins:
        cp.start()
    ins[0].wait()
    for l in range(LAYERS):
        for c in range(NC):
            for p in range(4):
                at = 384 * (2 * p + c % 2) + LANES * (c // 2)
                for y in range(Z):
                    OG[l, QUARTER * y:QUARTER * y + QUARTER, at:at + LANES] = GU[l, c, y, 0, :, LANES * p:LANES * p + LANES]
                    OU[l, QUARTER * y:QUARTER * y + QUARTER, at:at + LANES] = GU[l, c, y, 1, :, LANES * p:LANES * p + LANES]
    outs[parts].start()
    outs[parts + 1].start()
    ins[1].wait()
    for l in range(LAYERS):
        for j in range(3):
            for y in range(Z):
                OD[l, LANES * j:LANES * j + LANES, LANES * y:LANES * y + LANES] = DN[l, j, y].T
    outs[parts + 2].start()
    for i in range(parts):
        ins[2 + i].wait()
        outs[i].start()
    for cp in outs:
        cp.wait()


def solution(mesh, T=1024, TB=D):
    def step(x, dy, w_gate, w_up, w_down):
        N = x.shape[1]
        hbm = pl.BlockSpec(memory_space=pl.ANY)
        sds = jax.ShapeDtypeStruct
        v, dma = pltpu.VMEM, pltpu.SemaphoreType.DMA
        dx, ogu, od, *_ = pl.pallas_call(
            functools.partial(kernel, T, TB),
            name="step",
            out_shape=[
                sds((N, D), bf16), sds((LAYERS, NC, Z, 2, QUARTER, F), bf16), sds((LAYERS, 3, Z, LANES, LANES), bf16),
                sds((LAYERS, NC, 2, D, F), bf16), sds((LAYERS, NC, 4, 2, ROWS, D), bf16), sds((NC, 2, N, F), f32), sds((D, N), bf16),
            ],
            in_specs=[hbm] * 5,
            out_specs=[hbm] * 7,
            scratch_shapes=[
                v((N, D), bf16), v((D, N), bf16), v((N, D), bf16), v((D, N), bf16), v((N, D), bf16), v((N, D), f32),
                v((2, 3, D, D), bf16), v((2, 3, D, D), f32), v((2, 2, T, F), f32), v((NC, 2, ROWS, F), bf16),
                v((2, 4, ROWS, F), bf16), v((4, D, LANES), bf16), v((2, 2, 4, ROWS, F), bf16), v((4, D, LANES), bf16),
                v((2, 4, ROWS, F), bf16), v((4, D, LANES), bf16), v((2, ROWS, F), f32), v((D, LANES), f32), v((2, 2, 3, ROWS, F), bf16), v((3, D, LANES), bf16),
                v((2, 4, QUARTER, F), bf16), v((4, LANES, LANES), bf16), v((2, QUARTER, F), f32), v((LANES, LANES), f32), v((2, 2, 3, QUARTER, F), bf16), v((3, LANES, LANES), bf16),
                v((2, QUARTER, F), bf16), v((LANES, LANES), bf16),
                dma((NM,)), dma((3,)), dma((2,)), dma((2,)), *[dma((NM,)) for _ in range(7)], dma((3,)), dma((8, 3, 2)),
            ],
            compiler_params=pltpu.CompilerParams(collective_id=0, has_side_effects=True, vmem_limit_bytes=67043328),
        )(x[0], dy[0], w_gate, w_up, w_down)
        dx, *by_w = pl.pallas_call(
            deliver,
            name="deliver",
            out_shape=[sds((N, D), bf16), sds((LAYERS, ROWS, FF), bf16), sds((LAYERS, ROWS, FF), bf16), sds((LAYERS, 384, D), bf16)],
            in_specs=[hbm] * 3,
            out_specs=[hbm] * 4,
            scratch_shapes=[
                v((N, D), bf16), v((LAYERS, NC, Z, 2, QUARTER, F), bf16), v((LAYERS, 3, Z, LANES, LANES), bf16),
                v((LAYERS, ROWS, FF), bf16), v((LAYERS, ROWS, FF), bf16), v((LAYERS, 384, D), bf16), dma((6,)), dma((7,)),
            ],
            compiler_params=pltpu.CompilerParams(vmem_limit_bytes=67043328),
        )(dx, ogu, od)
        return dx[None], *by_w

    states, cut = P(("rep", "r", "s"), None, None), P(None, "s", None)
    return jax.shard_map(
        step,
        mesh=mesh,
        in_specs=(states, states) + (cut,) * 3,
        out_specs=(states,) + (P("rep", "s", None),) * 3,
        check_vma=False,
    )
```
